32 devices in a mesh: dom: 16 (over z, y, x), tp: 2 (over core).
Axes of the slice: x: 2, y: 2, z: 4, core: 2. Of those that a mesh axis runs over, the one named last changes fastest.
Arguments:
- node_latent: bfloat16 [16384, 128], P('dom'), may hold values from -6 to 6
- edge_latent: bfloat16 [131072, 128], P(('dom', 'tp')), may hold values from -6 to 6
- edge_sender: int32 [131072], P(('dom', 'tp')), may hold values from 0 to 1535, as said below
- edge_receiver: int32 [131072], P(('dom', 'tp')), may hold values from 0 to 1535, as said below
- edge_count: int32 [32], P(('dom', 'tp')), may hold values from 2048 to 4096, as said below
- send_index: int32 [16, 4, 128], P('dom'), may hold values from -1 to 1023, as said below
- edge_in: bfloat16 [3, 384, 128], P(None, None, 'tp'), may hold values from -0.3125 to 0.3125
- edge_out: bfloat16 [3, 128, 128], P(None, 'tp'), may hold values from -0.5 to 0.5
- node_in: bfloat16 [3, 256, 128], P(None, None, 'tp'), may hold values from -0.375 to 0.375
- node_out: bfloat16 [3, 128, 128], P(None, 'tp'), may hold values from -0.5 to 0.5
Outputs:
- node_result: bfloat16 [16384, 128], P('dom')
- edge_result: bfloat16 [131072, 128], P(('dom', 'tp'))
The draws below stay inside these ranges and needn't reach their ends.
Inputs may be any that keep to these rules, and one draw needn't show every extreme that they name: `send_index`: entry [p, k, j] is a local node index of partition p sent to partition (p + o_k) mod 16, with o = (1, -1, 2, -2); -1 marks padding, which stands only after the live entries of a block; live entries of a block are distinct; at least half of each block is live and some block is full. `edge_sender`: an index below 1024 is an owned node of the slot's partition; index 1024 + k * 128 + j is slot j of halo block k; never a padding halo slot. `edge_receiver`: as for edge_sender. `edge_count`: some device block is full.
All inputs are finite; a program needn't handle non-finite values.
Results may differ from the reference program's by a relative error of at most 0.013.
Values may be sent and summed in bfloat16 or wider, within the bound.
A program may use at most 64 MiB of HBM per device.

```python
import jax
import jax.numpy as jnp
from jax import lax

L = 128
H = 128
NODE_DEV = 1024
SLOT = 128
PEERS = 4
LAYERS = 3
EDGE_DEV = 4096
DOMAINS = 16
SHARDS = 32
NODES = 16384
EDGES = 131072


neighbour_offsets = (1, -1, 2, -2)


def halo_counts(key):
    counts = jax.random.randint(jax.random.fold_in(key, 11), (DOMAINS, PEERS), SLOT // 2, SLOT + 1)
    chosen = jax.random.randint(jax.random.fold_in(key, 12), (2,), 0, 1 << 20)
    counts = counts.at[chosen[0] % DOMAINS, chosen[1] % PEERS].set(SLOT)
    return counts.astype(jnp.int32)


def incoming_counts(key):
    counts = halo_counts(key)
    columns = [jnp.roll(counts[:, neighbour], offset) for neighbour, offset in enumerate(neighbour_offsets)]
    return jnp.stack(columns, axis=1)


def draw_send_index(key, part):
    counts = halo_counts(key)
    subkeys = jax.random.split(jax.random.fold_in(key, 13), DOMAINS * PEERS)
    chosen = jax.vmap(lambda subkey: jax.random.permutation(subkey, NODE_DEV)[:SLOT])(subkeys)
    chosen = chosen.reshape(DOMAINS, PEERS, SLOT)
    position = jnp.arange(SLOT, dtype=jnp.int32)[None, None, :]
    return jnp.where(position < counts[:, :, None], chosen, -1).astype(jnp.int32)


def endpoints(key, salt, halo_share):
    inbound = incoming_counts(key)
    base = jax.random.fold_in(key, salt)
    first_key, second_key, third_key, fourth_key = jax.random.split(base, 4)
    shape = (SHARDS, EDGE_DEV)
    owned_pick = jax.random.randint(first_key, shape, 0, NODE_DEV)
    block_pick = jax.random.randint(second_key, shape, 0, PEERS)
    raw_bits = jax.random.randint(third_key, shape, 0, 1 << 20)
    domain_of = (jnp.arange(SHARDS, dtype=jnp.int32) // (SHARDS // DOMAINS))[:, None]
    limit = inbound[domain_of, block_pick]
    halo_pick = NODE_DEV + block_pick * SLOT + raw_bits % limit
    use_halo = jax.random.randint(fourth_key, shape, 0, 100) < halo_share
    return jnp.where(use_halo, halo_pick, owned_pick).astype(jnp.int32).reshape(EDGES)


def draw_edge_sender(key, part):
    return endpoints(key, 21, 20)


def draw_edge_receiver(key, part):
    return endpoints(key, 22, 10)


def draw_edge_count(key, part):
    counts = jax.random.randint(jax.random.fold_in(key, 31), (SHARDS,), EDGE_DEV // 2, EDGE_DEV + 1)
    filled = jax.random.randint(jax.random.fold_in(key, 32), (), 0, SHARDS)
    return counts.at[filled].set(EDGE_DEV).astype(jnp.int32)


def block_levels(rng, dims, cuts, least, largest):
    level, own = 1.0, jax.random.fold_in(rng, 6)
    for axis_at, shards_of in cuts:
        heights = jnp.exp(jax.random.uniform(jax.random.fold_in(own, axis_at), (shards_of,), jnp.float32, least / len(cuts), largest / len(cuts)))
        level = level * jnp.repeat(heights, dims[axis_at] // shards_of).reshape([-1 if axis == axis_at else 1 for axis in range(len(dims))])
    return level


def bell_draw(rng, dims, width, bound, cuts=(), held_as=jnp.bfloat16):
    entries = jax.random.normal(rng, dims, jnp.float32) * width
    if len(cuts) > 0:
        entries = block_levels(rng, dims, cuts, -0.22, 0.18) * entries
    return jnp.clip(entries, min=-bound, max=bound).astype(held_as)


def setup_inputs(seed: int = 0) -> dict:
    arg_keys = jax.random.split(jax.random.key(seed), 11)
    node_latent = bell_draw(arg_keys[0], (NODES, L), 1.0, 6.0, ((0, 16),))
    edge_latent = bell_draw(arg_keys[1], (EDGES, L), 1.0, 6.0, ((0, 32),))
    edge_sender = draw_edge_sender(jax.random.fold_in(arg_keys[10], 71), 0)
    edge_receiver = draw_edge_receiver(jax.random.fold_in(arg_keys[10], 71), 0)
    edge_count = draw_edge_count(jax.random.fold_in(arg_keys[10], 71), 0)
    send_index = draw_send_index(jax.random.fold_in(arg_keys[10], 71), 0)
    edge_in = bell_draw(arg_keys[6], (LAYERS, 3 * L, H), (3 * L) ** -0.5, 0.3125, ((2, 2),))
    edge_out = bell_draw(arg_keys[7], (LAYERS, H, L), H ** -0.5, 0.5, ((1, 2),))
    node_in = bell_draw(arg_keys[8], (LAYERS, 2 * L, H), (2 * L) ** -0.5, 0.375, ((2, 2),))
    node_out = bell_draw(arg_keys[9], (LAYERS, H, L), H ** -0.5, 0.5, ((1, 2),))
    return {"node_latent": node_latent, "edge_latent": edge_latent, "edge_sender": edge_sender, "edge_receiver": edge_receiver, "edge_count": edge_count, "send_index": send_index, "edge_in": edge_in, "edge_out": edge_out, "node_in": node_in, "node_out": node_out}


neighbour_offsets = (1, -1, 2, -2)
norm_floor = 0.25

def layer_norm(values):
    centre = lax.optimization_barrier(jnp.mean(values, axis=-1, keepdims=True))
    centred = values - centre
    spread = lax.optimization_barrier(jnp.mean(centred * centred, axis=-1, keepdims=True))
    return centred * lax.rsqrt(spread + norm_floor)

def product(first_operand, second_operand):
    return jnp.dot(first_operand, second_operand, preferred_element_type=jnp.float32)

def reference(node_latent, edge_latent, edge_sender, edge_receiver, edge_count, send_index, edge_in, edge_out, node_in, node_out):
    feature_width = node_latent.shape[1]
    shard_count = SHARDS // DOMAINS
    extended_rows = NODE_DEV + PEERS * SLOT
    nodes_now = node_latent.reshape(DOMAINS, NODE_DEV, feature_width)
    edges_now = edge_latent.reshape(DOMAINS, shard_count * EDGE_DEV, feature_width)
    senders = edge_sender.reshape(DOMAINS, shard_count * EDGE_DEV)
    receivers = edge_receiver.reshape(DOMAINS, shard_count * EDGE_DEV)
    live_edges = (jnp.arange(EDGE_DEV, dtype=jnp.int32)[None, :] < edge_count[:, None]).reshape(DOMAINS, shard_count * EDGE_DEV)
    usable = send_index >= 0
    safe_index = jnp.where(usable, send_index, 0).astype(jnp.int32)
    domain_ids = jnp.arange(DOMAINS, dtype=jnp.int32)[:, None]
    for layer_index in range(LAYERS):
        picked = nodes_now[domain_ids[:, :, None], safe_index]
        picked = jnp.where(usable[..., None], picked, jnp.zeros((), jnp.bfloat16))
        halo_rows = jnp.stack([jnp.roll(picked[:, neighbour], offset, axis=0) for neighbour, offset in enumerate(neighbour_offsets)], axis=1)
        extended = jnp.concatenate([nodes_now, halo_rows.reshape(DOMAINS, PEERS * SLOT, feature_width)], axis=1)
        weight_in = edge_in[layer_index]
        weight_out = edge_out[layer_index]

        def edge_step(operands):
            extended_part, latent, sender_ids, receiver_ids, live_mask = operands
            linear = product(latent, weight_in[:feature_width])
            linear = linear + product(extended_part[sender_ids], weight_in[feature_width:2 * feature_width])
            linear = linear + product(extended_part[receiver_ids], weight_in[2 * feature_width:])
            edge_hidden = jnp.maximum(linear, 0.0).astype(jnp.bfloat16)
            message = jnp.where(live_mask[:, None], layer_norm(product(edge_hidden, weight_out)), 0.0).astype(jnp.bfloat16)
            message = lax.optimization_barrier(message)
            wide_message = message.astype(jnp.float32)
            renewed = (latent.astype(jnp.float32) + wide_message).astype(jnp.bfloat16)
            summed_part = jax.ops.segment_sum(wide_message, receiver_ids, num_segments=extended_rows)
            return (renewed, summed_part)
        edges_now, summed = lax.map(edge_step, (extended, edges_now, senders, receivers, live_edges))
        owned_sums = summed[:, :NODE_DEV]
        returned = summed[:, NODE_DEV:].reshape(DOMAINS, PEERS, SLOT, feature_width)
        for neighbour, offset in enumerate(neighbour_offsets):
            arrived = jnp.roll(returned[:, neighbour], -offset, axis=0)
            arrived = jnp.where(usable[:, neighbour, :, None], arrived, 0.0)
            owned_sums = owned_sums.at[domain_ids, safe_index[:, neighbour]].add(arrived)
        aggregate = owned_sums.astype(jnp.bfloat16).reshape(DOMAINS * NODE_DEV, feature_width)
        flat_nodes = nodes_now.reshape(DOMAINS * NODE_DEV, feature_width)
        first_weight = node_in[layer_index]
        linear_nodes = product(flat_nodes, first_weight[:feature_width]) + product(aggregate, first_weight[feature_width:])
        node_hidden = jnp.maximum(linear_nodes, 0.0).astype(jnp.bfloat16)
        update = layer_norm(product(node_hidden, node_out[layer_index]))
        nodes_now = (flat_nodes.astype(jnp.float32) + update).astype(jnp.bfloat16).reshape(DOMAINS, NODE_DEV, feature_width)
    return (nodes_now.reshape(NODES, feature_width), edges_now.reshape(EDGES, feature_width))
```

```python
import functools

import jax
import jax.numpy as jnp
from jax import lax
from jax.experimental import pallas as pl
from jax.experimental.pallas import tpu as pltpu
from jax.sharding import PartitionSpec as P

LAYERS = 3


neighbour_offsets = (1, -1, 2, -2)
norm_floor = 0.25


def from_behind(array, axis, by):
    length = lax.axis_size(axis)
    return lax.ppermute(array, axis, [(i, (i + by) % length) for i in range(length)])


def layer_norm(values):
    centre = jnp.mean(values, axis=-1, keepdims=True)
    centred = values - centre
    spread = jnp.mean(centred * centred, axis=-1, keepdims=True)
    return centred * lax.rsqrt(spread + norm_floor)


def product(first_operand, second_operand):
    return jnp.dot(first_operand, second_operand, preferred_element_type=jnp.float32)


def column_sum(table, values, exact):
    if exact:
        return lax.dot_general(
            table,
            values,
            (((0,), (0,)), ((), ())),
            precision=lax.Precision.HIGHEST,
            preferred_element_type=jnp.float32,
        )
    return lax.dot_general(
        table, values, (((0,), (0,)), ((), ())), preferred_element_type=jnp.float32
    )


def fetch_halo(nodes_now, pick_table):
    feature_width = nodes_now.shape[1]
    picked = (
        product(pick_table, nodes_now)
        .astype(jnp.bfloat16)
        .reshape(len(neighbour_offsets), -1, feature_width)
    )
    blocks = [
        from_behind(picked[neighbour], "dom", offset)
        for neighbour, offset in enumerate(neighbour_offsets)
    ]
    return jnp.concatenate(blocks, axis=0)


def return_sums(returned, pick_float, owned_sums):
    arrived = [
        from_behind(returned[neighbour].astype(jnp.bfloat16), "dom", -offset).astype(jnp.float32)
        for neighbour, offset in enumerate(neighbour_offsets)
    ]
    return owned_sums + column_sum(pick_float, jnp.concatenate(arrived, axis=0), True)


LOW = 256
BLOCK = 1024


def edge_kernel(
    count_ref, ext_ref, latent_ref, ids_ref, win_ref, wout_ref, renewed_ref, summed_ref,
    send_table, recv_table, sums,
):
    width = ext_ref.shape[1]
    high = ext_ref.shape[0] // LOW
    rows = latent_ref.shape[0]
    block = min(BLOCK, rows)
    for h in range(high):
        part = ext_ref[h * LOW : (h + 1) * LOW, :]
        lanes = slice(h * width, (h + 1) * width)
        send_table[:, lanes] = product(part, win_ref[width : 2 * width, :]).astype(jnp.bfloat16)
        recv_table[:, lanes] = product(part, win_ref[2 * width :, :]).astype(jnp.bfloat16)
    sums[...] = jnp.zeros_like(sums)
    weight_out = wout_ref[...]
    count = count_ref[0]

    def gathered(ids, table):
        low = ids & (LOW - 1)
        lane = lax.broadcasted_iota(jnp.int32, (block, width), 1)
        halves = [(low == lane + c).astype(jnp.bfloat16) for c in range(0, LOW, width)]
        all_rows = product(jnp.concatenate(halves, axis=1), table[...])
        top = ids // LOW
        found = all_rows[:, :width]
        for h in range(1, high):
            found = jnp.where(top == h, all_rows[:, h * width : (h + 1) * width], found)
        return found

    def step(i, carry):
        at = pl.ds(pl.multiple_of(i * block, block), block)
        send_row = ids_ref[0:1, at]
        recv_row = ids_ref[1:2, at]
        send_ids = jnp.broadcast_to(send_row, (width, block)).T
        recv_ids = jnp.broadcast_to(recv_row, (width, block)).T
        latent = latent_ref[at, :]
        linear = product(latent, win_ref[:width, :])
        linear = linear + gathered(send_ids, send_table) + gathered(recv_ids, recv_table)
        hidden = jnp.maximum(linear, 0.0).astype(jnp.bfloat16)
        message = layer_norm(product(hidden, weight_out))
        position = lax.broadcasted_iota(jnp.int32, (block, width), 0) + i * block
        message = jnp.where(position < count, message, 0.0).astype(jnp.bfloat16)
        wide = message.astype(jnp.float32)
        renewed_ref[at, :] = (latent.astype(jnp.float32) + wide).astype(jnp.bfloat16)
        top = recv_ids // LOW
        spread = jnp.concatenate(
            [jnp.where(top == h, wide, 0.0).astype(jnp.bfloat16) for h in range(high)], axis=1
        )
        low_row = jnp.broadcast_to(recv_row & (LOW - 1), (LOW, block))
        table = (low_row == lax.broadcasted_iota(jnp.int32, (LOW, block), 0)).astype(jnp.bfloat16)
        sums[...] += product(table, spread)
        return carry

    lax.fori_loop(0, rows // block, step, 0)
    for h in range(high):
        summed_ref[h * LOW : (h + 1) * LOW, :] = sums[:, h * width : (h + 1) * width]


def edge_stage(extended, edges_now, id_rows, edge_count, weight_in, weight_out):
    total, width = extended.shape
    rows = edges_now.shape[0]
    high = total // LOW
    whole = pl.BlockSpec(memory_space=pltpu.VMEM)
    return pl.pallas_call(
        edge_kernel,
        out_shape=(
            jax.ShapeDtypeStruct((rows, width), jnp.bfloat16),
            jax.ShapeDtypeStruct((total, width), jnp.float32),
        ),
        in_specs=[pl.BlockSpec(memory_space=pltpu.SMEM)] + [whole] * 5,
        out_specs=(whole, whole),
        scratch_shapes=[
            pltpu.VMEM((LOW, high * width), jnp.bfloat16),
            pltpu.VMEM((LOW, high * width), jnp.bfloat16),
            pltpu.VMEM((LOW, high * width), jnp.float32),
        ],
        compiler_params=pltpu.CompilerParams(vmem_limit_bytes=48 * 1024 * 1024),
        cost_estimate=pl.CostEstimate(
            flops=8 * rows * total * width, bytes_accessed=4 * rows * width, transcendentals=rows
        ),
    )(edge_count, extended, edges_now, id_rows, weight_in, weight_out)


def local(
    node_latent,
    edge_latent,
    edge_sender,
    edge_receiver,
    edge_count,
    send_index,
    edge_in,
    edge_out,
    node_in,
    node_out,
):
    feature_width = node_latent.shape[1]
    node_total = node_latent.shape[0]
    share_rows = node_total // lax.axis_size("tp")
    first_row = lax.axis_index("tp") * share_rows
    flat_index = send_index[0].reshape(-1)
    halo_total = flat_index.shape[0]
    extended_total = node_total + halo_total
    pick_match = flat_index[:, None] == jnp.arange(node_total, dtype=jnp.int32)[None, :]
    pick_table = pick_match.astype(jnp.bfloat16)
    pick_float = pick_match.astype(jnp.float32)
    id_rows = jnp.stack([edge_sender, edge_receiver])
    full_in, full_out = (
        lax.all_gather(edge_in, "tp", axis=2, tiled=True),
        lax.all_gather(edge_out, "tp", axis=1, tiled=True),
    )
    node_first, node_second = (
        lax.all_gather(node_in, "tp", axis=2, tiled=True),
        lax.all_gather(node_out, "tp", axis=1, tiled=True),
    )
    nodes_now = node_latent
    edges_now = edge_latent
    for layer_index in range(LAYERS):
        halo_rows = fetch_halo(nodes_now, pick_table)
        extended = jnp.concatenate([nodes_now, halo_rows], axis=0)
        edges_now, summed = edge_stage(
            extended, edges_now, id_rows, edge_count, full_in[layer_index], full_out[layer_index]
        )
        returned = summed[node_total:].reshape(len(neighbour_offsets), -1, feature_width)
        owned_sums = return_sums(returned, pick_float, summed[:node_total])
        share_sum = lax.psum_scatter(owned_sums, "tp", scatter_dimension=0, tiled=True)
        aggregate = share_sum.astype(jnp.bfloat16)
        own_rows = lax.dynamic_slice_in_dim(nodes_now, first_row, share_rows, 0)
        linear_nodes = product(own_rows, node_first[layer_index][:feature_width]) + product(
            aggregate, node_first[layer_index][feature_width:]
        )
        node_hidden = jnp.maximum(linear_nodes, 0.0).astype(jnp.bfloat16)
        update = product(node_hidden, node_second[layer_index])
        renewed = (own_rows.astype(jnp.float32) + layer_norm(update)).astype(jnp.bfloat16)
        nodes_now = lax.all_gather(renewed, "tp", axis=0, tiled=True)
    return (nodes_now, edges_now)


def solution(mesh):
    return jax.shard_map(
        local,
        mesh=mesh,
        in_specs=(
            P("dom", None),
            P(("dom", "tp"), None),
            P(("dom", "tp")),
            P(("dom", "tp")),
            P(("dom", "tp")),
            P("dom", None, None),
            P(None, None, "tp"),
            P(None, "tp", None),
            P(None, None, "tp"),
            P(None, "tp", None),
        ),
        out_specs=(P("dom", None), P(("dom", "tp"), None)),
        check_vma=False,
    )
```

```python
import functools

import jax
import jax.numpy as jnp
from jax import lax
from jax.experimental import pallas as pl
from jax.experimental.pallas import tpu as pltpu
from jax.sharding import PartitionSpec as P

LAYERS = 3


neighbour_offsets = (1, -1, 2, -2)
norm_floor = 0.25


def layer_norm(values):
    centre = jnp.mean(values, axis=-1, keepdims=True)
    centred = values - centre
    spread = jnp.mean(centred * centred, axis=-1, keepdims=True)
    return centred * lax.rsqrt(spread + norm_floor)


def product(first_operand, second_operand):
    return jnp.dot(first_operand, second_operand, preferred_element_type=jnp.float32)


MESH = pl.DeviceIdType.MESH
PEERS = len(neighbour_offsets)


def peer_ids(size):
    me = lax.axis_index("dom")
    return [{"dom": lax.rem(me + offset + size, size)} for offset in neighbour_offsets]


def partner_id():
    return {"tp": 1 - lax.axis_index("tp")}


def greet(size):
    barrier = pltpu.get_barrier_semaphore()
    everyone = peer_ids(size) + [partner_id()]
    for device in everyone:
        pl.semaphore_signal(barrier, inc=1, device_id=device, device_id_type=MESH)
    pl.semaphore_wait(barrier, len(everyone))


def send(source, target, sems, at, device):
    copy = pltpu.make_async_remote_copy(
        src_ref=source,
        dst_ref=target,
        send_sem=sems.at[0, at],
        recv_sem=sems.at[1, at],
        device_id=device,
        device_id_type=MESH,
    )
    copy.start()
    return copy


def fill_pick(index_ref, pick, node_total):
    slots = index_ref.shape[1]
    wanted = jnp.broadcast_to(index_ref[...], (128, slots)).T
    lane = lax.broadcasted_iota(jnp.int32, (slots, 128), 1)
    for c in range(0, node_total, 128):
        pick[:, c : c + 128] = (wanted == lane + c).astype(jnp.bfloat16)


def start_halo(size, nodes, pick, extended_ref, outgoing, incoming, sems):
    node_total = nodes.shape[0]
    slot = pick.shape[0] // PEERS
    for k in range(PEERS):
        outgoing[k] = product(pick[k * slot : (k + 1) * slot, :], nodes).astype(jnp.bfloat16)
    extended_ref[:node_total, :] = nodes
    peers = peer_ids(size)
    return [send(outgoing.at[k], incoming.at[k], sems, k, peers[k]) for k in range(PEERS)]


def finish_halo(copies, extended_ref, incoming):
    slot = incoming.shape[1]
    first = extended_ref.shape[0] - PEERS * slot
    for k, copy in enumerate(copies):
        copy.wait()
        extended_ref[first + k * slot : first + (k + 1) * slot, :] = incoming[k]


def start_kernel(size, *refs):
    nodes_ref, index_ref = refs[:2]
    halves = refs[2:6]
    extended_ref = refs[6]
    fulls = refs[7:11]
    others = refs[11:15]
    outgoing, incoming, pick, halo_sems, weight_sems = refs[15:]
    greet(size)
    weight_copies = [
        send(half, other, weight_sems, i, partner_id())
        for i, (half, other) in enumerate(zip(halves, others))
    ]
    fill_pick(index_ref, pick, nodes_ref.shape[0])
    copies = start_halo(size, nodes_ref[...], pick, extended_ref, outgoing, incoming, halo_sems)
    mine = lax.axis_index("tp")
    for half, other, full, copy in zip(halves, others, fulls, weight_copies):
        copy.wait()
        layers, rows, columns = half.shape
        for layer in range(layers):
            if columns < full.shape[2]:
                shape = (columns, full.shape[2])
                gap = lax.broadcasted_iota(jnp.int32, shape, 1)
                gap = gap - lax.broadcasted_iota(jnp.int32, shape, 0)
                own_place = (gap == mine * columns).astype(jnp.bfloat16)
                far_place = (gap == (1 - mine) * columns).astype(jnp.bfloat16)
                joined = product(half[layer], own_place) + product(other[layer], far_place)
                full[layer] = joined.astype(jnp.bfloat16)
            else:
                near, far = half[layer], other[layer]
                full[layer, :rows, :] = jnp.where(mine == 0, near, far)
                full[layer, rows:, :] = jnp.where(mine == 0, far, near)
    finish_halo(copies, extended_ref, incoming)


def node_kernel(size, more, *refs):
    extended_ref, own_ref, back_ref, index_ref, win_ref, wout_ref, result_ref = refs[:7]
    own_far, back_near, back_far, sums_sems, table = refs[7:12]
    node_total, width = own_ref.shape
    slots = index_ref.shape[1]
    slot = slots // PEERS
    peers = peer_ids(size)
    opposite = [neighbour_offsets.index(-offset) for offset in neighbour_offsets]
    greet(size)
    own_copy = send(own_ref, own_far, sums_sems, 0, partner_id())
    back_copies = [
        send(
            back_ref.at[pl.ds(k * slot, slot), :], back_near.at[pl.ds(k * slot, slot), :],
            sums_sems, 1 + k, peers[opposite[k]],
        )
        for k in range(PEERS)
    ]
    wanted = jnp.broadcast_to(index_ref[...], (128, slots))
    row = lax.broadcasted_iota(jnp.int32, (128, slots), 0)
    for c in range(0, node_total, 128):
        table[c : c + 128, :] = (wanted == row + c).astype(jnp.bfloat16)
    if more:
        outgoing, incoming, pick, halo_sems = refs[12:]
        fill_pick(index_ref, pick, node_total)
    nodes = extended_ref[:node_total, :]
    linear = product(nodes, win_ref[:width, :])
    far_copies = []
    for k in range(PEERS):
        back_copies[k].wait()
        rows = pl.ds(k * slot, slot)
        far_copies.append(
            send(back_near.at[rows, :], back_far.at[rows, :], sums_sems, 1 + PEERS + k, partner_id())
        )
    arrived = product(table[...], back_near[...])
    own_copy.wait()
    owned = own_ref[...] + own_far[...]
    for copy in far_copies:
        copy.wait()
    owned = owned + (arrived + product(table[...], back_far[...]))
    linear = linear + product(owned.astype(jnp.bfloat16), win_ref[width:, :])
    hidden = jnp.maximum(linear, 0.0).astype(jnp.bfloat16)
    update = layer_norm(product(hidden, wout_ref[...]))
    nodes = (nodes.astype(jnp.float32) + update).astype(jnp.bfloat16)
    if more:
        copies = start_halo(size, nodes, pick, result_ref, outgoing, incoming, halo_sems)
        finish_halo(copies, result_ref, incoming)
    else:
        result_ref[...] = nodes


def halo_scratch(node_total, slots, width):
    return [
        pltpu.VMEM((PEERS, slots // PEERS, width), jnp.bfloat16),
        pltpu.VMEM((PEERS, slots // PEERS, width), jnp.bfloat16),
        pltpu.VMEM((slots, node_total), jnp.bfloat16),
        pltpu.SemaphoreType.DMA((2, PEERS)),
    ]


def start_stage(nodes, index_row, halves):
    node_total, width = nodes.shape
    slots = index_row.shape[1]
    whole = pl.BlockSpec(memory_space=pltpu.VMEM)
    parts = lax.axis_size("tp")
    fulls = []
    for axis, half in zip((2, 1, 2, 1), halves):
        shape = list(half.shape)
        shape[axis] *= parts
        fulls.append(jax.ShapeDtypeStruct(tuple(shape), half.dtype))
    extended = jax.ShapeDtypeStruct((node_total + slots, width), nodes.dtype)
    return pl.pallas_call(
        functools.partial(start_kernel, lax.axis_size("dom")),
        out_shape=(extended, *fulls),
        in_specs=[whole] * 6,
        out_specs=(whole,) * 5,
        scratch_shapes=[pltpu.VMEM(half.shape, half.dtype) for half in halves]
        + halo_scratch(node_total, slots, width)
        + [pltpu.SemaphoreType.DMA((2, 4))],
        compiler_params=pltpu.CompilerParams(
            collective_id=0, has_side_effects=True, vmem_limit_bytes=40 * 1024 * 1024
        ),
    )(nodes, index_row, *halves)


def node_stage(more, extended, own, back, index_row, weight_in, weight_out):
    node_total, width = own.shape
    slots = index_row.shape[1]
    whole = pl.BlockSpec(memory_space=pltpu.VMEM)
    rows = node_total + slots if more else node_total
    scratch = [
        pltpu.VMEM((node_total, width), jnp.float32),
        pltpu.VMEM((slots, width), jnp.bfloat16),
        pltpu.VMEM((slots, width), jnp.bfloat16),
        pltpu.SemaphoreType.DMA((2, 1 + 2 * PEERS)),
        pltpu.VMEM((node_total, slots), jnp.bfloat16),
    ]
    if more:
        scratch = scratch + halo_scratch(node_total, slots, width)
    return pl.pallas_call(
        functools.partial(node_kernel, lax.axis_size("dom"), more),
        out_shape=jax.ShapeDtypeStruct((rows, width), extended.dtype),
        in_specs=[whole] * 6,
        out_specs=whole,
        scratch_shapes=scratch,
        compiler_params=pltpu.CompilerParams(
            collective_id=1 if more else 2,
            has_side_effects=True,
            vmem_limit_bytes=40 * 1024 * 1024,
        ),
    )(extended, own, back, index_row, weight_in, weight_out)


LOW = 256
BLOCK = 1024


def edge_kernel(
    count_ref, ext_ref, latent_ref, ids_ref, win_ref, wout_ref, renewed_ref, own_ref, back_ref,
    send_table, recv_table, sums,
):
    width = ext_ref.shape[1]
    high = ext_ref.shape[0] // LOW
    rows = latent_ref.shape[0]
    block = min(BLOCK, rows)
    for h in range(high):
        part = ext_ref[h * LOW : (h + 1) * LOW, :]
        lanes = slice(h * width, (h + 1) * width)
        send_table[:, lanes] = product(part, win_ref[width : 2 * width, :]).astype(jnp.bfloat16)
        recv_table[:, lanes] = product(part, win_ref[2 * width :, :]).astype(jnp.bfloat16)
    sums[...] = jnp.zeros_like(sums)
    weight_out = wout_ref[...]
    count = count_ref[0]

    def gathered(ids, table):
        low = ids & (LOW - 1)
        lane = lax.broadcasted_iota(jnp.int32, (block, width), 1)
        halves = [(low == lane + c).astype(jnp.bfloat16) for c in range(0, LOW, width)]
        all_rows = product(jnp.concatenate(halves, axis=1), table[...])
        top = ids // LOW
        found = all_rows[:, :width]
        for h in range(1, high):
            found = jnp.where(top == h, all_rows[:, h * width : (h + 1) * width], found)
        return found

    def step(i, carry):
        at = pl.ds(pl.multiple_of(i * block, block), block)
        send_row = ids_ref[0:1, at]
        recv_row = ids_ref[1:2, at]
        send_ids = jnp.broadcast_to(send_row, (width, block)).T
        recv_ids = jnp.broadcast_to(recv_row, (width, block)).T
        latent = latent_ref[at, :]
        linear = product(latent, win_ref[:width, :])
        linear = linear + gathered(send_ids, send_table) + gathered(recv_ids, recv_table)
        hidden = jnp.maximum(linear, 0.0).astype(jnp.bfloat16)
        message = layer_norm(product(hidden, weight_out))
        position = lax.broadcasted_iota(jnp.int32, (block, width), 0) + i * block
        message = jnp.where(position < count, message, 0.0).astype(jnp.bfloat16)
        wide = message.astype(jnp.float32)
        renewed_ref[at, :] = (latent.astype(jnp.float32) + wide).astype(jnp.bfloat16)
        top = recv_ids // LOW
        spread = jnp.concatenate(
            [jnp.where(top == h, wide, 0.0).astype(jnp.bfloat16) for h in range(high)], axis=1
        )
        low_row = jnp.broadcast_to(recv_row & (LOW - 1), (LOW, block))
        table = (low_row == lax.broadcasted_iota(jnp.int32, (LOW, block), 0)).astype(jnp.bfloat16)
        sums[...] += product(table, spread)
        return carry

    lax.fori_loop(0, rows // block, step, 0)
    for h in range(high):
        part = sums[:, h * width : (h + 1) * width]
        at = h * LOW
        if at < own_ref.shape[0]:
            own_ref[at : at + LOW, :] = part
        else:
            at = at - own_ref.shape[0]
            back_ref[at : at + LOW, :] = part.astype(jnp.bfloat16)


def edge_stage(node_total, extended, edges_now, id_rows, edge_count, weight_in, weight_out):
    total, width = extended.shape
    rows = edges_now.shape[0]
    high = total // LOW
    whole = pl.BlockSpec(memory_space=pltpu.VMEM)
    return pl.pallas_call(
        edge_kernel,
        out_shape=(
            jax.ShapeDtypeStruct((rows, width), jnp.bfloat16),
            jax.ShapeDtypeStruct((node_total, width), jnp.float32),
            jax.ShapeDtypeStruct((total - node_total, width), jnp.bfloat16),
        ),
        in_specs=[pl.BlockSpec(memory_space=pltpu.SMEM)] + [whole] * 5,
        out_specs=(whole, whole, whole),
        scratch_shapes=[
            pltpu.VMEM((LOW, high * width), jnp.bfloat16),
            pltpu.VMEM((LOW, high * width), jnp.bfloat16),
            pltpu.VMEM((LOW, high * width), jnp.float32),
        ],
        compiler_params=pltpu.CompilerParams(vmem_limit_bytes=48 * 1024 * 1024),
        cost_estimate=pl.CostEstimate(
            flops=8 * rows * total * width, bytes_accessed=4 * rows * width, transcendentals=rows
        ),
    )(edge_count, extended, edges_now, id_rows, weight_in, weight_out)


def local(
    node_latent,
    edge_latent,
    edge_sender,
    edge_receiver,
    edge_count,
    send_index,
    edge_in,
    edge_out,
    node_in,
    node_out,
):
    node_total = node_latent.shape[0]
    index_row = send_index.reshape(1, -1)
    id_rows = jnp.stack([edge_sender, edge_receiver])
    current, full_in, full_out, node_first, node_second = start_stage(
        node_latent, index_row, (edge_in, edge_out, node_in, node_out)
    )
    edges_now = edge_latent
    for layer in range(LAYERS):
        edges_now, own, back = edge_stage(
            node_total, current, edges_now, id_rows, edge_count, full_in[layer], full_out[layer]
        )
        more = layer + 1 < LAYERS
        current = node_stage(
            more, current, own, back, index_row, node_first[layer], node_second[layer]
        )
    return (current, edges_now)


def solution(mesh):
    return jax.shard_map(
        local,
        mesh=mesh,
        in_specs=(
            P("dom", None),
            P(("dom", "tp"), None),
            P(("dom", "tp")),
            P(("dom", "tp")),
            P(("dom", "tp")),
            P("dom", None, None),
            P(None, None, "tp"),
            P(None, "tp", None),
            P(None, None, "tp"),
            P(None, "tp", None),
        ),
        out_specs=(P("dom", None), P(("dom", "tp"), None)),
        check_vma=False,
    )
```

```python
import functools

import jax
import jax.numpy as jnp
from jax import lax
from jax.experimental import pallas as pl
from jax.experimental.pallas import tpu as pltpu
from jax.sharding import PartitionSpec as P

LAYERS = 3


neighbour_offsets = (1, -1, 2, -2)
norm_floor = 0.25


def layer_norm(values):
    centre = jnp.mean(values, axis=-1, keepdims=True)
    centred = values - centre
    spread = jnp.mean(centred * centred, axis=-1, keepdims=True)
    return centred * lax.rsqrt(spread + norm_floor)


def product(first_operand, second_operand):
    return jnp.dot(first_operand, second_operand, preferred_element_type=jnp.float32)


MESH = pl.DeviceIdType.MESH
PEERS = len(neighbour_offsets)


def peer_ids(size):
    me = lax.axis_index("dom")
    return [{"dom": lax.rem(me + offset + size, size)} for offset in neighbour_offsets]


def partner_id():
    return {"tp": 1 - lax.axis_index("tp")}


def greet(size):
    barrier = pltpu.get_barrier_semaphore()
    everyone = peer_ids(size) + [partner_id()]
    for device in everyone:
        pl.semaphore_signal(barrier, inc=1, device_id=device, device_id_type=MESH)
    pl.semaphore_wait(barrier, len(everyone))


def send(source, target, sems, at, device):
    copy = pltpu.make_async_remote_copy(
        src_ref=source,
        dst_ref=target,
        send_sem=sems.at[0, at],
        recv_sem=sems.at[1, at],
        device_id=device,
        device_id_type=MESH,
    )
    copy.start()
    return copy


def fill_pick(index_ref, pick, node_total):
    slots = index_ref.shape[1]
    wanted = jnp.broadcast_to(index_ref[...], (128, slots)).T
    lane = lax.broadcasted_iota(jnp.int32, (slots, 128), 1)
    for c in range(0, node_total, 128):
        pick[:, c : c + 128] = (wanted == lane + c).astype(jnp.bfloat16)


def join_halves(mine, half, other, full):
    layers, rows, columns = half.shape
    for layer in range(layers):
        if columns < full.shape[2]:
            shape = (columns, full.shape[2])
            gap = lax.broadcasted_iota(jnp.int32, shape, 1)
            gap = gap - lax.broadcasted_iota(jnp.int32, shape, 0)
            own_place = (gap == mine * columns).astype(jnp.bfloat16)
            far_place = (gap == (1 - mine) * columns).astype(jnp.bfloat16)
            joined = product(half[layer], own_place) + product(other[layer], far_place)
            full[layer] = joined.astype(jnp.bfloat16)
        else:
            near, far = half[layer], other[layer]
            full[layer, :rows, :] = jnp.where(mine == 0, near, far)
            full[layer, rows:, :] = jnp.where(mine == 0, far, near)


LOW = 256
BLOCK = 1024


def kernel(size, *refs):
    count_ref, nodes_in, latent_ref, sender_ref, receiver_ref, index_ref = refs[:6]
    halves, refs = refs[6:10], refs[10:]
    nodes_ref, edges_ref = refs[:2]
    others, fulls, refs = refs[2:6], refs[6:10], refs[10:]
    outgoing, halo_in, back_out, back_near, back_far, own_sums, own_far = refs[:7]
    pick, place, low_hot, tops, recv_hot, linear, messages = refs[7:14]
    send_table, recv_table, back_sums, sems, weight_sems = refs[14:]
    edge_in, edge_out, node_in, node_out = fulls
    node_total, width = nodes_ref.shape
    rows = edges_ref.shape[0]
    slots = index_ref.shape[1]
    slot = slots // PEERS
    own_high, high = node_total // LOW, (node_total + slots) // LOW
    block = min(BLOCK, rows)
    peers = peer_ids(size)
    opposite = [neighbour_offsets.index(-offset) for offset in neighbour_offsets]
    partner = partner_id()
    mine = lax.axis_index("tp")
    per_layer = 2 + 3 * PEERS
    own_group = own_high // 2

    def each_block(body):
        def step(i, carry):
            body(pl.multiple_of(i * block, block))
            return carry

        lax.fori_loop(0, rows // block, step, 0)

    def send_halo(layer, nodes):
        base = layer * per_layer
        for k in range(PEERS):
            part = product(pick[k * slot : (k + 1) * slot, :], nodes)
            outgoing[layer, k * slot : (k + 1) * slot, :] = part.astype(jnp.bfloat16)
        nodes_ref[...] = nodes
        copies = []
        for k in range(PEERS):
            at = pl.ds(k * slot, slot)
            copies.append(
                send(outgoing.at[layer, at], halo_in.at[layer, at], sems, base + k, peers[k])
            )
        return copies

    def fill_tables(layer, part, h):
        lanes = slice(h * width, (h + 1) * width)
        weight = edge_in[layer]
        send_table[:, lanes] = product(part, weight[width : 2 * width, :]).astype(jnp.bfloat16)
        recv_table[:, lanes] = product(part, weight[2 * width :, :]).astype(jnp.bfloat16)

    def gathered(side, at, table, first, last):
        found_rows = product(
            low_hot[side, pl.ds(at, block), :], table[:, first * width : last * width]
        )
        top = tops[side, pl.ds(at, block), :]
        found = jnp.zeros((block, width), jnp.float32)
        for h in range(first, last):
            lanes = slice((h - first) * width, (h - first + 1) * width)
            found = jnp.where(top == h, found_rows[:, lanes], found)
        return found

    def scattered(at, message, first, last):
        wide = message.astype(jnp.float32)
        top = tops[1, pl.ds(at, block), :]
        spread = [
            jnp.where(top == h, wide, 0.0).astype(jnp.bfloat16) for h in range(first, last)
        ]
        return product(recv_hot[:, pl.ds(at, block)], jnp.concatenate(spread, axis=1))

    greet(size)
    weight_copies = [
        send(half, other, weight_sems, i, partner)
        for i, (half, other) in enumerate(zip(halves, others))
    ]
    fill_pick(index_ref, pick, node_total)
    halo_copies = send_halo(0, nodes_in[...])
    wanted = jnp.broadcast_to(index_ref[...], (128, slots))
    row = lax.broadcasted_iota(jnp.int32, (128, slots), 0)
    for c in range(0, node_total, 128):
        place[c : c + 128, :] = (wanted == row + c).astype(jnp.bfloat16)
    for half, other, full, copy in zip(halves, others, fulls, weight_copies):
        copy.wait()
        join_halves(mine, half, other, full)

    def prepare(at):
        here = pl.ds(at, block)
        for side, ids_ref in enumerate((sender_ref, receiver_ref)):
            ids = jnp.broadcast_to(ids_ref[0:1, here], (width, block)).T
            low = ids & (LOW - 1)
            lane = lax.broadcasted_iota(jnp.int32, (block, width), 1)
            for c in range(0, LOW, width):
                low_hot[side, here, c : c + width] = (low == lane + c).astype(jnp.bfloat16)
            tops[side, here, :] = ids // LOW
        low_row = jnp.broadcast_to(receiver_ref[0:1, here] & (LOW - 1), (LOW, block))
        down = lax.broadcasted_iota(jnp.int32, (LOW, block), 0)
        recv_hot[:, here] = (low_row == down).astype(jnp.bfloat16)
        linear[here, :] = product(latent_ref[here, :], edge_in[0, :width, :])

    each_block(prepare)
    for layer in range(LAYERS):
        base = layer * per_layer
        more = layer + 1 < LAYERS
        latents = latent_ref if layer == 0 else edges_ref
        for h in range(own_high):
            fill_tables(layer, nodes_ref[h * LOW : (h + 1) * LOW, :], h)

        def own_gather(at):
            here = pl.ds(at, block)
            found = gathered(0, at, send_table, 0, own_high)
            linear[here, :] += found + gathered(1, at, recv_table, 0, own_high)

        each_block(own_gather)
        for copy in halo_copies:
            copy.wait()
        for h in range(own_high, high):
            at = (h - own_high) * LOW
            fill_tables(layer, halo_in[layer, at : at + LOW, :], h)
        back_sums[...] = jnp.zeros_like(back_sums)

        def finish_edges(at):
            here = pl.ds(at, block)
            found = linear[here, :] + gathered(0, at, send_table, own_high, high)
            found = found + gathered(1, at, recv_table, own_high, high)
            hidden = jnp.maximum(found, 0.0).astype(jnp.bfloat16)
            message = layer_norm(product(hidden, edge_out[layer]))
            position = lax.broadcasted_iota(jnp.int32, (block, width), 0) + at
            message = jnp.where(position < count_ref[0], message, 0.0).astype(jnp.bfloat16)
            messages[here, :] = message
            renewed = latents[here, :].astype(jnp.float32) + message.astype(jnp.float32)
            edges_ref[here, :] = renewed.astype(jnp.bfloat16)
            back_sums[...] += scattered(at, message, own_high, high)

        each_block(finish_edges)
        for h in range(own_high, high):
            at = (h - own_high) * LOW
            lanes = slice(at // LOW * width, (at // LOW + 1) * width)
            back_out[layer, at : at + LOW, :] = back_sums[:, lanes].astype(jnp.bfloat16)
        own_sums[layer] = jnp.zeros(own_sums.shape[1:], jnp.float32)
        back_copies = []
        for k in range(PEERS):
            at = pl.ds(k * slot, slot)
            back_copies.append(
                send(
                    back_out.at[layer, at], back_near.at[layer, at],
                    sems, base + PEERS + k, peers[opposite[k]],
                )
            )
        own_copies = []
        for group in range(2):
            first = group * own_group

            def own_scatter(at):
                message = messages[pl.ds(at, block), :]
                own_sums[layer, group] += scattered(at, message, first, first + own_group)

            each_block(own_scatter)
            own_copies.append(
                send(
                    own_sums.at[layer, group], own_far.at[layer, group],
                    sems, base + 3 * PEERS + group, partner,
                )
            )
        far_copies = []
        for k in range(PEERS):
            back_copies[k].wait()
            at = pl.ds(k * slot, slot)
            far_copies.append(
                send(
                    back_near.at[layer, at], back_far.at[layer, at],
                    sems, base + 2 * PEERS + k, partner,
                )
            )
        if more:

            def next_linear(at):
                here = pl.ds(at, block)
                linear[here, :] = product(edges_ref[here, :], edge_in[layer + 1, :width, :])

            each_block(next_linear)
        nodes = nodes_ref[...]
        arrived = product(place[...], back_near[layer])
        weight = node_in[layer]
        hidden = product(nodes, weight[:width, :])
        for copy in own_copies:
            copy.wait()
        owned = []
        for h in range(own_high):
            group, at = h // own_group, (h % own_group) * width
            near = own_sums[layer, group, :, at : at + width]
            owned.append(near + own_far[layer, group, :, at : at + width])
        for copy in far_copies:
            copy.wait()
        arrived = arrived + product(place[...], back_far[layer])
        aggregate = (jnp.concatenate(owned, axis=0) + arrived).astype(jnp.bfloat16)
        hidden = hidden + product(aggregate, weight[width:, :])
        hidden = jnp.maximum(hidden, 0.0).astype(jnp.bfloat16)
        update = layer_norm(product(hidden, node_out[layer]))
        nodes = (nodes.astype(jnp.float32) + update).astype(jnp.bfloat16)
        if more:
            halo_copies = send_halo(layer + 1, nodes)
        else:
            nodes_ref[...] = nodes


def local(
    node_latent,
    edge_latent,
    edge_sender,
    edge_receiver,
    edge_count,
    send_index,
    edge_in,
    edge_out,
    node_in,
    node_out,
):
    node_total, width = node_latent.shape
    rows = edge_latent.shape[0]
    index_row = send_index.reshape(1, -1)
    slots = index_row.shape[1]
    parts = lax.axis_size("tp")
    halves = (edge_in, edge_out, node_in, node_out)
    fulls = []
    for axis, half in zip((2, 1, 2, 1), halves):
        shape = list(half.shape)
        shape[axis] *= parts
        fulls.append(tuple(shape))
    narrow, total = jnp.bfloat16, node_total + slots
    own_group = (LAYERS, 2, LOW, node_total // LOW // 2 * width)
    scratch = [pltpu.VMEM(half.shape, half.dtype) for half in halves]
    scratch += [pltpu.VMEM(shape, narrow) for shape in fulls]
    scratch += [pltpu.VMEM((LAYERS, slots, width), narrow) for _ in range(5)]
    scratch += [
        pltpu.VMEM(own_group, jnp.float32),
        pltpu.VMEM(own_group, jnp.float32),
        pltpu.VMEM((slots, node_total), narrow),
        pltpu.VMEM((node_total, slots), narrow),
        pltpu.VMEM((2, rows, LOW), narrow),
        pltpu.VMEM((2, rows, width), jnp.int32),
        pltpu.VMEM((LOW, rows), narrow),
        pltpu.VMEM((rows, width), jnp.float32),
        pltpu.VMEM((rows, width), narrow),
        pltpu.VMEM((LOW, total // LOW * width), narrow),
        pltpu.VMEM((LOW, total // LOW * width), narrow),
        pltpu.VMEM((LOW, slots // LOW * width), jnp.float32),
        pltpu.SemaphoreType.DMA((2, LAYERS * (2 + 3 * PEERS))),
        pltpu.SemaphoreType.DMA((2, len(halves))),
    ]
    whole = pl.BlockSpec(memory_space=pltpu.VMEM)
    return pl.pallas_call(
        functools.partial(kernel, lax.axis_size("dom")),
        out_shape=(
            jax.ShapeDtypeStruct((node_total, width), narrow),
            jax.ShapeDtypeStruct((rows, width), narrow),
        ),
        in_specs=[pl.BlockSpec(memory_space=pltpu.SMEM)] + [whole] * 9,
        out_specs=(whole, whole),
        scratch_shapes=scratch,
        compiler_params=pltpu.CompilerParams(
            collective_id=0, has_side_effects=True, vmem_limit_bytes=48 * 1024 * 1024
        ),
    )(
        edge_count,
        node_latent,
        edge_latent,
        edge_sender.reshape(1, rows),
        edge_receiver.reshape(1, rows),
        index_row,
        *halves,
    )


def solution(mesh):
    return jax.shard_map(
        local,
        mesh=mesh,
        in_specs=(
            P("dom", None),
            P(("dom", "tp"), None),
            P(("dom", "tp")),
            P(("dom", "tp")),
            P(("dom", "tp")),
            P("dom", None, None),
            P(None, None, "tp"),
            P(None, "tp", None),
            P(None, None, "tp"),
            P(None, "tp", None),
        ),
        out_specs=(P("dom", None), P(("dom", "tp"), None)),
        check_vma=False,
    )
```

```python
import functools

import jax
import jax.numpy as jnp
from jax import lax
from jax.experimental import pallas as pl
from jax.experimental.pallas import tpu as pltpu
from jax.sharding import PartitionSpec as P

LAYERS = 3


neighbour_offsets = (1, -1, 2, -2)
norm_floor = 0.25


def layer_norm(values):
    centre = jnp.mean(values, axis=-1, keepdims=True)
    centred = values - centre
    spread = jnp.mean(centred * centred, axis=-1, keepdims=True)
    return centred * lax.rsqrt(spread + norm_floor)


def product(first_operand, second_operand):
    return jnp.dot(first_operand, second_operand, preferred_element_type=jnp.float32)


MESH = pl.DeviceIdType.MESH
PEERS = len(neighbour_offsets)


def peer_ids(size):
    me = lax.axis_index("dom")
    return [{"dom": lax.rem(me + offset + size, size)} for offset in neighbour_offsets]


def partner_id():
    return {"tp": 1 - lax.axis_index("tp")}


def greet(size):
    barrier = pltpu.get_barrier_semaphore()
    everyone = peer_ids(size) + [partner_id()]
    for device in everyone:
        pl.semaphore_signal(barrier, inc=1, device_id=device, device_id_type=MESH)
    pl.semaphore_wait(barrier, len(everyone))


def send(source, target, sems, at, device):
    copy = pltpu.make_async_remote_copy(
        src_ref=source,
        dst_ref=target,
        send_sem=sems.at[0, at],
        recv_sem=sems.at[1, at],
        device_id=device,
        device_id_type=MESH,
    )
    copy.start()
    return copy


def fill_pick(index_ref, pick, node_total):
    slots = index_ref.shape[1]
    wanted = jnp.broadcast_to(index_ref[...], (128, slots)).T
    lane = lax.broadcasted_iota(jnp.int32, (slots, 128), 1)
    for c in range(0, node_total, 128):
        pick[:, c : c + 128] = (wanted == lane + c).astype(jnp.bfloat16)


def join_halves(mine, half, other, full):
    layers, rows, columns = half.shape
    for layer in range(layers):
        if columns < full.shape[2]:
            shape = (columns, full.shape[2])
            gap = lax.broadcasted_iota(jnp.int32, shape, 1)
            gap = gap - lax.broadcasted_iota(jnp.int32, shape, 0)
            own_place = (gap == mine * columns).astype(jnp.bfloat16)
            far_place = (gap == (1 - mine) * columns).astype(jnp.bfloat16)
            joined = product(half[layer], own_place) + product(other[layer], far_place)
            full[layer] = joined.astype(jnp.bfloat16)
        else:
            near, far = half[layer], other[layer]
            full[layer, :rows, :] = jnp.where(mine == 0, near, far)
            full[layer, rows:, :] = jnp.where(mine == 0, far, near)


def double_block(weight):
    gap = jnp.zeros_like(weight)
    top = jnp.concatenate([weight, gap], axis=1)
    return jnp.concatenate([top, jnp.concatenate([gap, weight], axis=1)], axis=0)


def paired_product(values, doubled):
    rows, width = values.shape
    pairs = jnp.concatenate([values[: rows // 2], values[rows // 2 :]], axis=1)
    out = product(pairs, doubled)
    return jnp.concatenate([out[:, :width], out[:, width:]], axis=0)


def unit_spread(centred):
    spread = jnp.mean(centred * centred, axis=-1, keepdims=True)
    return centred * lax.rsqrt(spread + norm_floor)


LOW = 256
BLOCK = 4096


def kernel(size, *refs):
    count_ref, nodes_in, latent_ref, sender_ref, receiver_ref, index_ref = refs[:6]
    halves, refs = refs[6:10], refs[10:]
    nodes_ref, edges_ref = refs[:2]
    others, fulls, refs = refs[2:6], refs[6:10], refs[10:]
    outgoing, halo_in, back_out, back_near, back_far, own_sums, own_far = refs[:7]
    pick, place, low_hot, tops, recv_hot, linear, messages = refs[7:14]
    send_table, recv_table, back_sums, out_pair, sems, weight_sems = refs[14:]
    edge_in, edge_out, node_in, node_out = fulls
    node_total, width = nodes_ref.shape
    rows = edges_ref.shape[0]
    slots = index_ref.shape[1]
    slot = slots // PEERS
    own_high, high = node_total // LOW, (node_total + slots) // LOW
    block = min(BLOCK, rows)
    peers = peer_ids(size)
    opposite = [neighbour_offsets.index(-offset) for offset in neighbour_offsets]
    partner = partner_id()
    mine = lax.axis_index("tp")
    per_layer = 2 + 3 * PEERS
    own_group = own_high // 2

    def each_block(body):
        def step(i, carry):
            body(pl.multiple_of(i * block, block))
            return carry

        lax.fori_loop(0, rows // block, step, 0)

    def send_halo(layer, nodes):
        base = layer * per_layer
        for k in range(PEERS):
            part = product(pick[k * slot : (k + 1) * slot, :], nodes)
            outgoing[layer, k * slot : (k + 1) * slot, :] = part.astype(jnp.bfloat16)
        nodes_ref[...] = nodes
        copies = []
        for k in range(PEERS):
            at = pl.ds(k * slot, slot)
            copies.append(
                send(outgoing.at[layer, at], halo_in.at[layer, at], sems, base + k, peers[k])
            )
        return copies

    def fill_tables(layer, part, h):
        lanes = slice(h * width, (h + 1) * width)
        weight = edge_in[layer]
        send_table[:, lanes] = product(part, weight[width : 2 * width, :]).astype(jnp.bfloat16)
        recv_table[:, lanes] = product(part, weight[2 * width :, :]).astype(jnp.bfloat16)

    def gathered(side, at, table, first, last):
        found_rows = product(
            low_hot[side, pl.ds(at, block), :], table[:, first * width : last * width]
        )
        top = tops[side, pl.ds(at, block), :]
        found = jnp.zeros((block, width), jnp.float32)
        for h in range(first, last):
            lanes = slice((h - first) * width, (h - first + 1) * width)
            found = jnp.where(top == h, found_rows[:, lanes], found)
        return found

    def scattered(at, message, first, last):
        wide = message.astype(jnp.float32)
        top = tops[1, pl.ds(at, block), :]
        spread = [
            jnp.where(top == h, wide, 0.0).astype(jnp.bfloat16) for h in range(first, last)
        ]
        return product(recv_hot[:, pl.ds(at, block)], jnp.concatenate(spread, axis=1))

    greet(size)
    weight_copies = [
        send(half, other, weight_sems, i, partner)
        for i, (half, other) in enumerate(zip(halves, others))
    ]
    fill_pick(index_ref, pick, node_total)
    halo_copies = send_halo(0, nodes_in[...])
    wanted = jnp.broadcast_to(index_ref[...], (128, slots))
    row = lax.broadcasted_iota(jnp.int32, (128, slots), 0)
    for c in range(0, node_total, 128):
        place[c : c + 128, :] = (wanted == row + c).astype(jnp.bfloat16)
    for half, other, full, copy in zip(halves, others, fulls, weight_copies):
        copy.wait()
        join_halves(mine, half, other, full)

    def prepare(at):
        here = pl.ds(at, block)
        for side, ids_ref in enumerate((sender_ref, receiver_ref)):
            ids = jnp.broadcast_to(ids_ref[0:1, here], (width, block)).T
            low = ids & (LOW - 1)
            lane = lax.broadcasted_iota(jnp.int32, (block, width), 1)
            for c in range(0, LOW, width):
                low_hot[side, here, c : c + width] = (low == lane + c).astype(jnp.bfloat16)
            tops[side, here, :] = ids // LOW
        low_row = jnp.broadcast_to(receiver_ref[0:1, here] & (LOW - 1), (LOW, block))
        down = lax.broadcasted_iota(jnp.int32, (LOW, block), 0)
        recv_hot[:, here] = (low_row == down).astype(jnp.bfloat16)
        linear[here, :] = product(latent_ref[here, :], edge_in[0, :width, :])

    each_block(prepare)
    for layer in range(LAYERS):
        base = layer * per_layer
        more = layer + 1 < LAYERS
        latents = latent_ref if layer == 0 else edges_ref
        second = edge_out[layer].astype(jnp.float32)
        second = second - jnp.mean(second, axis=1, keepdims=True)
        out_pair[layer] = double_block(second.astype(jnp.bfloat16))
        for h in range(own_high):
            fill_tables(layer, nodes_ref[h * LOW : (h + 1) * LOW, :], h)

        def own_gather(at):
            here = pl.ds(at, block)
            found = gathered(0, at, send_table, 0, own_high)
            linear[here, :] += found + gathered(1, at, recv_table, 0, own_high)

        each_block(own_gather)
        for copy in halo_copies:
            copy.wait()
        for h in range(own_high, high):
            at = (h - own_high) * LOW
            fill_tables(layer, halo_in[layer, at : at + LOW, :], h)
        back_sums[...] = jnp.zeros_like(back_sums)

        def finish_edges(at):
            here = pl.ds(at, block)
            found = linear[here, :] + gathered(0, at, send_table, own_high, high)
            found = found + gathered(1, at, recv_table, own_high, high)
            hidden = jnp.maximum(found, 0.0).astype(jnp.bfloat16)
            message = unit_spread(paired_product(hidden, out_pair[layer]))
            position = lax.broadcasted_iota(jnp.int32, (block, width), 0) + at
            message = jnp.where(position < count_ref[0], message, 0.0).astype(jnp.bfloat16)
            messages[here, :] = message
            renewed = latents[here, :].astype(jnp.float32) + message.astype(jnp.float32)
            edges_ref[here, :] = renewed.astype(jnp.bfloat16)
            back_sums[...] += scattered(at, message, own_high, high)

        each_block(finish_edges)
        for h in range(own_high, high):
            at = (h - own_high) * LOW
            lanes = slice(at // LOW * width, (at // LOW + 1) * width)
            back_out[layer, at : at + LOW, :] = back_sums[:, lanes].astype(jnp.bfloat16)
        own_sums[layer] = jnp.zeros(own_sums.shape[1:], jnp.float32)
        back_copies = []
        for k in range(PEERS):
            at = pl.ds(k * slot, slot)
            back_copies.append(
                send(
                    back_out.at[layer, at], back_near.at[layer, at],
                    sems, base + PEERS + k, peers[opposite[k]],
                )
            )
        own_copies = []
        for group in range(2):
            first = group * own_group

            def own_scatter(at):
                message = messages[pl.ds(at, block), :]
                own_sums[layer, group] += scattered(at, message, first, first + own_group)

            each_block(own_scatter)
            own_copies.append(
                send(
                    own_sums.at[layer, group], own_far.at[layer, group],
                    sems, base + 3 * PEERS + group, partner,
                )
            )
        far_copies = []
        for k in range(PEERS):
            back_copies[k].wait()
            at = pl.ds(k * slot, slot)
            far_copies.append(
                send(
                    back_near.at[layer, at], back_far.at[layer, at],
                    sems, base + 2 * PEERS + k, partner,
                )
            )
        if more:

            def next_linear(at):
                here = pl.ds(at, block)
                linear[here, :] = product(edges_ref[here, :], edge_in[layer + 1, :width, :])

            each_block(next_linear)
        nodes = nodes_ref[...]
        arrived = product(place[...], back_near[layer])
        weight = node_in[layer]
        hidden = product(nodes, weight[:width, :])
        for copy in own_copies:
            copy.wait()
        owned = []
        for h in range(own_high):
            group, at = h // own_group, (h % own_group) * width
            near = own_sums[layer, group, :, at : at + width]
            owned.append(near + own_far[layer, group, :, at : at + width])
        for copy in far_copies:
            copy.wait()
        arrived = arrived + product(place[...], back_far[layer])
        aggregate = (jnp.concatenate(owned, axis=0) + arrived).astype(jnp.bfloat16)
        hidden = hidden + product(aggregate, weight[width:, :])
        hidden = jnp.maximum(hidden, 0.0).astype(jnp.bfloat16)
        update = layer_norm(product(hidden, node_out[layer]))
        nodes = (nodes.astype(jnp.float32) + update).astype(jnp.bfloat16)
        if more:
            halo_copies = send_halo(layer + 1, nodes)
        else:
            nodes_ref[...] = nodes


def local(
    node_latent,
    edge_latent,
    edge_sender,
    edge_receiver,
    edge_count,
    send_index,
    edge_in,
    edge_out,
    node_in,
    node_out,
):
    node_total, width = node_latent.shape
    rows = edge_latent.shape[0]
    index_row = send_index.reshape(1, -1)
    slots = index_row.shape[1]
    parts = lax.axis_size("tp")
    halves = (edge_in, edge_out, node_in, node_out)
    fulls = []
    for axis, half in zip((2, 1, 2, 1), halves):
        shape = list(half.shape)
        shape[axis] *= parts
        fulls.append(tuple(shape))
    narrow, total = jnp.bfloat16, node_total + slots
    own_group = (LAYERS, 2, LOW, node_total // LOW // 2 * width)
    scratch = [pltpu.VMEM(half.shape, half.dtype) for half in halves]
    scratch += [pltpu.VMEM(shape, narrow) for shape in fulls]
    scratch += [pltpu.VMEM((LAYERS, slots, width), narrow) for _ in range(5)]
    scratch += [
        pltpu.VMEM(own_group, jnp.float32),
        pltpu.VMEM(own_group, jnp.float32),
        pltpu.VMEM((slots, node_total), narrow),
        pltpu.VMEM((node_total, slots), narrow),
        pltpu.VMEM((2, rows, LOW), narrow),
        pltpu.VMEM((2, rows, width), jnp.int32),
        pltpu.VMEM((LOW, rows), narrow),
        pltpu.VMEM((rows, width), jnp.float32),
        pltpu.VMEM((rows, width), narrow),
        pltpu.VMEM((LOW, total // LOW * width), narrow),
        pltpu.VMEM((LOW, total // LOW * width), narrow),
        pltpu.VMEM((LOW, slots // LOW * width), jnp.float32),
        pltpu.VMEM((LAYERS, 2 * width, 2 * width), narrow),
        pltpu.SemaphoreType.DMA((2, LAYERS * (2 + 3 * PEERS))),
        pltpu.SemaphoreType.DMA((2, len(halves))),
    ]
    whole = pl.BlockSpec(memory_space=pltpu.VMEM)
    return pl.pallas_call(
        functools.partial(kernel, lax.axis_size("dom")),
        out_shape=(
            jax.ShapeDtypeStruct((node_total, width), narrow),
            jax.ShapeDtypeStruct((rows, width), narrow),
        ),
        in_specs=[pl.BlockSpec(memory_space=pltpu.SMEM)] + [whole] * 9,
        out_specs=(whole, whole),
        scratch_shapes=scratch,
        compiler_params=pltpu.CompilerParams(
            collective_id=0, has_side_effects=True, vmem_limit_bytes=48 * 1024 * 1024
        ),
    )(
        edge_count,
        node_latent,
        edge_latent,
        edge_sender.reshape(1, rows),
        edge_receiver.reshape(1, rows),
        index_row,
        *halves,
    )


def solution(mesh):
    return jax.shard_map(
        local,
        mesh=mesh,
        in_specs=(
            P("dom", None),
            P(("dom", "tp"), None),
            P(("dom", "tp")),
            P(("dom", "tp")),
            P(("dom", "tp")),
            P("dom", None, None),
            P(None, None, "tp"),
            P(None, "tp", None),
            P(None, None, "tp"),
            P(None, "tp", None),
        ),
        out_specs=(P("dom", None), P(("dom", "tp"), None)),
        check_vma=False,
    )
```
